32 devices in a mesh: replica: 4 (over y, x), fsdp: 8 (over z, core).
Axes of the slice: x: 2, y: 2, z: 4, core: 2. Of those that a mesh axis runs over, the one named last changes fastest.
Arguments:
- base_weights: float32 [8192, 1024], P('fsdp'), may hold values from -5 to 5, as said below
- inner_weights: bfloat16 [4, 8192, 1024], P('replica', 'fsdp'), may hold values from -12 to 12, as said below
- momentum: float32 [8192, 1024], P(('fsdp', 'replica')), may hold values from -1 to 1
Outputs:
- new_base: float32 [8192, 1024], P('fsdp')
- new_momentum: float32 [8192, 1024], P(('fsdp', 'replica'))
- new_inner: bfloat16 [4, 8192, 1024], P('replica', 'fsdp')
The draws below stay inside these ranges and needn't reach their ends.
Inputs may be any that keep to these rules, and one draw needn't show every extreme that they name: `base_weights`: the shared outer weights, multiples of 2 ** -16. `inner_weights`: each replica's weights after its inner steps, multiples of 2 ** -16.
All inputs are finite; a program needn't handle non-finite values.
Results may differ from the reference program's by a relative error of at most 0.0015.
Values may be sent and summed in bfloat16 or wider, within the bound.
A program may use at most 64 MiB of HBM per device.

```python
import jax
import jax.numpy as jnp
from jax import lax

D = 8192
KVW = 1024
BLOCK = 128
REPLICAS = 4


grid_step = 65536.0


def draw_common(key):
    folded = jax.random.fold_in(key, 11)
    base_key = jax.random.fold_in(folded, 0)
    column_key = jax.random.fold_in(folded, 1)
    own_key = jax.random.fold_in(folded, 2)
    row_key = jax.random.fold_in(folded, 4)
    base_values = jnp.clip(jax.random.normal(base_key, (D, KVW), jnp.float32), -5.0, 5.0)
    base_values = jnp.floor(base_values * grid_step + 0.5) / grid_step
    columns = jnp.exp(jax.random.uniform(column_key, (KVW,), jnp.float32, 0.0, jnp.log(10.0)))
    row_scale = 0.1 * jnp.exp(jax.random.uniform(row_key, (D,), jnp.float32, -jnp.log(1000.0), 0.0))
    copies = jnp.exp(jnp.log(3.0) * jnp.arange(REPLICAS, dtype=jnp.float32) / (REPLICAS - 1))
    own_noise = jax.random.uniform(own_key, (REPLICAS, D, KVW), jnp.float32, -1.0, 1.0)
    perturb = own_noise
    deltas = perturb * row_scale[None, :, None] * columns[None, None, :] * copies[:, None, None]
    inner_values = base_values[None] - deltas
    inner_values = jnp.floor(inner_values * grid_step + 0.5) / grid_step
    return (base_values, inner_values)


def draw_base_weights(key, part):
    base_values, inner_values = draw_common(key)
    return base_values.astype(jnp.float32)


def draw_inner_weights(key, part):
    base_values, inner_values = draw_common(key)
    return inner_values.astype(jnp.bfloat16)


def levels(key, dims, pieces, low, top_value):
    def one(axis_at, parts):
        draws = jax.random.uniform(jax.random.fold_in(jax.random.fold_in(key, 6), axis_at), (parts,), jnp.float32, low / len(pieces), top_value / len(pieces))
        return jnp.repeat(jnp.exp(draws), dims[axis_at] // parts).reshape((-1,) + (1,) * (len(dims) - axis_at - 1))

    gain = one(*pieces[0])
    for cut in pieces[1:]:
        gain = gain * one(*cut)
    return gain


def scatter_about(key, dims, spread, most, pieces=(), held_as=jnp.bfloat16):
    factor_of = levels(key, dims, pieces, -0.22, 0.18) if pieces else 1.0
    array = jax.random.normal(key, dims, jnp.float32) * spread * factor_of
    return jnp.minimum(jnp.maximum(array, -most), most).astype(held_as)


def setup_inputs(seed: int = 0) -> dict:
    key_of = jax.random.split(jax.random.key(seed), 4)
    return {
        "base_weights": draw_base_weights(jax.random.fold_in(key_of[3], 71), 0),
        "inner_weights": draw_inner_weights(jax.random.fold_in(key_of[3], 71), 0),
        "momentum": scatter_about(key_of[2], (D, KVW), 0.2, 1.0, ((0, 32),), jnp.float32),
    }


code_limit = 448.0
outer_rate = 0.7
outer_momentum = 0.9
blend_share = 0.5
clip_rms = 0.02
epsilon = 1e-06
smallest_normal = 0.015625

def power_two(exponent):
    unit_ones = jnp.ones_like(exponent)
    upward = jnp.left_shift(unit_ones, jnp.maximum(exponent, 0)).astype(jnp.float32)
    downward = jnp.left_shift(unit_ones, jnp.maximum(-exponent, 0)).astype(jnp.float32)
    return upward / downward

def exponent_above(target):
    estimate = jnp.ceil(jnp.log2(target)).astype(jnp.int32)
    estimate = jnp.where(target <= power_two(estimate - 1), estimate - 1, estimate)
    return jnp.where(target > power_two(estimate), estimate + 1, estimate)

def exponent_below(target):
    estimate = jnp.floor(jnp.log2(target)).astype(jnp.int32)
    estimate = jnp.where(target >= power_two(estimate + 1), estimate + 1, estimate)
    return jnp.where(target < power_two(estimate), estimate - 1, estimate)

def encode(deltas):
    shaped = deltas.reshape(deltas.shape[0], deltas.shape[1] // BLOCK, BLOCK)
    block_peaks = lax.optimization_barrier(jnp.max(jnp.abs(shaped), axis=2))
    scales = power_two(exponent_above((block_peaks + epsilon) / code_limit))
    code_units = shaped / scales[:, :, None]
    magnitude = jnp.abs(code_units)
    quantum = power_two(exponent_below(jnp.maximum(magnitude, smallest_normal)) - 3)
    steps_count = jnp.floor(magnitude / quantum + 0.5)
    code_values = (jnp.where(code_units < 0, -steps_count, steps_count) * quantum).astype(jnp.bfloat16)
    return (code_values, scales)

def reference(base_weights, inner_weights, momentum):

    def add_replica(summed, replica_copy):
        deltas = base_weights - replica_copy.astype(jnp.float32)
        code_values, scales = encode(deltas)
        decoded = code_values.astype(jnp.float32) * scales[:, :, None]
        return (summed + decoded.reshape(deltas.shape), None)
    summed, unused = lax.scan(add_replica, jnp.zeros(base_weights.shape, jnp.float32), inner_weights)
    outer_grad = summed / REPLICAS
    grad_sq = jnp.sum(outer_grad * outer_grad)
    clip_factor = jnp.minimum(1.0, clip_rms / jnp.sqrt(grad_sq / (D * KVW) + epsilon))
    step_term = clip_factor * outer_grad
    new_momentum = outer_momentum * momentum + step_term
    new_base = base_weights - outer_rate * (step_term + outer_momentum * new_momentum)

    def blend_one(replica_copy):
        blended = blend_share * replica_copy.astype(jnp.float32) + (1.0 - blend_share) * new_base
        return blended.astype(jnp.bfloat16)
    new_inner = lax.map(blend_one, inner_weights)
    return (new_base, new_momentum, new_inner)
```

```python
import functools

import jax
import jax.numpy as jnp
from jax import lax
from jax.experimental import pallas as pl
from jax.experimental.pallas import tpu as pltpu
from jax.sharding import PartitionSpec as P

BLOCK = 128
HALF_GROUPS = 2

code_limit = 448.0
outer_rate = 0.7
outer_momentum = 0.9
blend_share = 0.5
clip_rms = 0.02
epsilon = 1e-06

MESH = pl.DeviceIdType.MESH


def decoded_deltas(deltas):
    peaks = jnp.max(jnp.abs(deltas), axis=1, keepdims=True) + epsilon
    rough = peaks * (1.0 / code_limit)
    wide = rough * (2.0**23 + 1.0)
    power = wide - (wide - rough)
    scales = jnp.where(power * code_limit < peaks, power + power, power)
    nudged = deltas * (1.0 + 2.0**-23)
    wide_deltas = nudged * (2.0**20 + 1.0)
    four_bits = wide_deltas - (wide_deltas - nudged)
    shift = scales * (1.5 * 2.0**14)
    fixed_step = (nudged + shift) - shift
    return jnp.where(jnp.abs(deltas) < scales * 2.0**-6, fixed_step, four_bits)


def grid_sides(replicas):
    side = 1 << (replicas.bit_length() // 2)
    while replicas % side:
        side -= 1
    return side, replicas // side


def kernel(
    dims,
    base_hbm, inner_hbm, momentum_hbm,
    new_base, new_momentum, new_inner,
    base_v, inner_v, momentum_v, dec, first, second, grad, update,
    square_mine, square_near, square_row, square_far,
    load_sems, send_one, recv_one, send_two, recv_two, send_all, recv_all,
    near_send, near_recv, far_send, far_recv,
):
    replicas, shards_count, rows, columns, groups, total = dims
    width = columns // groups
    span_x, span_y = grid_sides(replicas)
    tile = min(32, rows)
    me = lax.axis_index("replica")
    row_me = lax.axis_index("fsdp")
    me_x, me_y = lax.rem(me, span_x), me // span_x

    def spans(g):
        return (span_x, span_y) if g % 2 == 0 else (span_y, span_x)

    def owner(g, dp, dq):
        dx, dy = (dp, dq) if g % 2 == 0 else (dq, dp)
        return lax.rem(me_y + dy, span_y) * span_x + lax.rem(me_x + dx, span_x)

    def near(step):
        return lax.rem(me + step, replicas)

    def far(step):
        return lax.rem(row_me + step, shards_count)

    def row_start(index):
        return pl.multiple_of(index * rows, rows)

    load_order = [(dx, dy) for dy in reversed(range(span_y)) for dx in reversed(range(span_x))]
    loads = []
    for at, (dx, dy) in enumerate(load_order):
        here = pl.ds(row_start(owner(0, dx, dy)), rows)
        pair = (
            pltpu.make_async_copy(base_hbm.at[here], base_v.at[here], load_sems.at[at, 0]),
            pltpu.make_async_copy(inner_hbm.at[0, here], inner_v.at[here], load_sems.at[at, 1]),
        )
        for copy in pair:
            copy.start()
        loads.append(pair)
    momentum_load = pltpu.make_async_copy(momentum_hbm, momentum_v, load_sems.at[replicas, 0])
    momentum_load.start()

    barrier = pltpu.get_barrier_semaphore()
    for step in range(1, replicas):
        pl.semaphore_signal(barrier, inc=1, device_id={"replica": near(step)}, device_id_type=MESH)
    for step in range(1, shards_count):
        pl.semaphore_signal(barrier, inc=1, device_id={"fsdp": far(step)}, device_id_type=MESH)

    def encode(g, dp, dq):
        slot = dp * spans(g)[1] + dq
        start = row_start(owner(g, dp, dq))

        @pl.loop(0, rows // tile)
        def _(t):
            at = pl.ds(pl.multiple_of(start + t * tile, tile), tile)
            to = pl.ds(pl.multiple_of(t * tile, tile), tile)
            for c in range(0, width, BLOCK):
                cols = pl.ds(g * width + c, BLOCK)
                deltas = base_v[at, cols] - inner_v[at, cols].astype(jnp.float32)
                dec[g, slot, to, pl.ds(c, BLOCK)] = decoded_deltas(deltas).astype(jnp.bfloat16)

    def copy_one(g, dp, dq):
        slot = dp * spans(g)[1] + dq
        return pltpu.make_async_remote_copy(
            src_ref=dec.at[g, slot], dst_ref=first.at[g, slot],
            send_sem=send_one.at[g, slot], recv_sem=recv_one.at[g, slot],
            device_id={"replica": owner(g, dp, 0)}, device_id_type=MESH,
        )

    def copy_two(g, dq):
        return pltpu.make_async_remote_copy(
            src_ref=dec.at[g, dq], dst_ref=second.at[g, dq],
            send_sem=send_two.at[g, dq], recv_sem=recv_two.at[g, dq],
            device_id={"replica": owner(g, 0, dq)}, device_id_type=MESH,
        )

    def copy_all(g, dp, dq, source):
        np, nq = spans(g)
        slot = ((np - dp) % np) * nq + (source if dp else (nq - dq) % nq)
        return pltpu.make_async_remote_copy(
            src_ref=update.at[g, source if dp else 0], dst_ref=update.at[g, slot],
            send_sem=send_all.at[g, slot], recv_sem=recv_all.at[g, slot],
            device_id={"replica": owner(g, dp, dq)}, device_id_type=MESH,
        )

    waited = set()

    def await_load(g, dp, dq):
        key = (dp, dq) if g % 2 == 0 else (dq, dp)
        if key not in waited:
            waited.add(key)
            for copy in loads[load_order.index(key)]:
                copy.wait()

    sends = []
    greeted = False
    most = max(span_x, span_y)
    for dq in reversed(range(most)):
        for dp in reversed(range(1, most)):
            for g in range(groups):
                np, nq = spans(g)
                if dp < np and dq < nq:
                    await_load(g, dp, dq)
                    encode(g, dp, dq)
                    if not greeted:
                        pl.semaphore_wait(barrier, replicas - 1 + shards_count - 1)
                        greeted = True
                    copy = copy_one(g, dp, dq)
                    copy.start()
                    sends.append(copy)
    for dq in reversed(range(most)):
        for g in range(groups):
            if dq < spans(g)[1]:
                await_load(g, 0, dq)
                encode(g, 0, dq)

    for dq in reversed(range(most)):
        for g in range(groups):
            np, nq = spans(g)
            if dq >= nq:
                continue
            for dp in range(1, np):
                copy_one(g, dp, dq).wait_recv()

            @pl.loop(0, rows // tile)
            def _(t):
                at = pl.ds(pl.multiple_of(t * tile, tile), tile)
                summed = dec[g, dq, at].astype(jnp.float32)
                for dp in range(1, np):
                    summed += first[g, dp * nq + dq, at].astype(jnp.float32)
                if dq:
                    dec[g, dq, at] = summed.astype(jnp.bfloat16)
                else:
                    grad[at, pl.ds(g * width, width)] = summed

            if dq:
                copy = copy_two(g, dq)
                copy.start()
                sends.append(copy)

    squares = jnp.zeros((8, BLOCK), jnp.float32)
    for g in range(groups):
        nq = spans(g)[1]
        for dq in range(1, nq):
            copy_two(g, dq).wait_recv()

        def add(t, squares):
            at = pl.ds(pl.multiple_of(t * tile, tile), tile)
            for c in range(0, width, BLOCK):
                cols = pl.ds(g * width + c, BLOCK)
                summed = grad[at, cols]
                for dq in range(1, nq):
                    summed += second[g, dq, at, pl.ds(c, BLOCK)].astype(jnp.float32)
                outer = summed * (1.0 / replicas)
                grad[at, cols] = outer
                square = outer * outer
                for s in range(0, tile, 8):
                    squares += square[s : s + 8]
            return squares

        squares = lax.fori_loop(0, rows // tile, add, squares)

    square_mine[...] = squares
    near_copies = []
    for step in range(1, replicas):
        copy = pltpu.make_async_remote_copy(
            src_ref=square_mine, dst_ref=square_near.at[step],
            send_sem=near_send.at[step], recv_sem=near_recv.at[step],
            device_id={"replica": near(step)}, device_id_type=MESH,
        )
        copy.start()
        near_copies.append(copy)
    sends += near_copies
    for copy in near_copies:
        copy.wait_recv()
    for step in range(1, replicas):
        squares += square_near[step]
    square_row[...] = squares
    far_copies = []
    for step in range(1, shards_count):
        copy = pltpu.make_async_remote_copy(
            src_ref=square_row, dst_ref=square_far.at[step],
            send_sem=far_send.at[step], recv_sem=far_recv.at[step],
            device_id={"fsdp": far(step)}, device_id_type=MESH,
        )
        copy.start()
        far_copies.append(copy)
    sends += far_copies
    momentum_load.wait()
    for copy in far_copies:
        copy.wait_recv()
    for step in range(1, shards_count):
        squares += square_far[step]
    mean_square = jnp.full((1, BLOCK), jnp.sum(squares), jnp.float32) / total
    clip_factor = jnp.minimum(1.0, clip_rms / jnp.sqrt(mean_square + epsilon))

    for g in range(groups):
        np, nq = spans(g)

        @pl.loop(0, rows // tile)
        def _(t):
            at = pl.ds(pl.multiple_of(t * tile, tile), tile)
            for c in range(0, width, BLOCK):
                cols = pl.ds(g * width + c, BLOCK)
                step_term = clip_factor * grad[at, cols]
                moved = outer_momentum * momentum_v[at, cols] + step_term
                new_momentum[at, cols] = moved
                update[g, 0, at, pl.ds(c, BLOCK)] = (step_term + outer_momentum * moved).astype(
                    jnp.bfloat16
                )

        for dq in range(1, nq):
            copy = copy_all(g, 0, dq, 0)
            copy.start()
            sends.append(copy)
    for g in range(groups):
        for dp in range(1, spans(g)[0]):
            copy = copy_all(g, dp, 0, 0)
            copy.start()
            sends.append(copy)

    def finish(g, dp, dq):
        slot = dp * spans(g)[1] + dq
        start = row_start(owner(g, dp, dq))

        @pl.loop(0, rows // tile)
        def _(t):
            at = pl.ds(pl.multiple_of(start + t * tile, tile), tile)
            to = pl.ds(pl.multiple_of(t * tile, tile), tile)
            cols = pl.ds(g * width, width)
            fresh = base_v[at, cols] - outer_rate * update[g, slot, to].astype(jnp.float32)
            new_base[at, cols] = fresh
            blended = blend_share * inner_v[at, cols].astype(jnp.float32) + (
                1.0 - blend_share
            ) * fresh
            new_inner[0, at, cols] = blended.astype(jnp.bfloat16)

    for g in range(groups):
        finish(g, 0, 0)
    for g in range(groups):
        np, nq = spans(g)
        for dq in range(1, nq):
            copy_all(g, 0, (nq - dq) % nq, 0).wait_recv()
            for dp in range(1, np):
                copy = copy_all(g, dp, 0, dq)
                copy.start()
                sends.append(copy)
            finish(g, 0, dq)
    for dq in range(most):
        for g in range(groups):
            np, nq = spans(g)
            if dq < nq:
                for dp in range(1, np):
                    copy_all(g, (np - dp) % np, 0, dq).wait_recv()
                    finish(g, dp, dq)
    for copy in sends:
        copy.wait_send()


def shards(base_weights, inner_weights, momentum):
    replicas = lax.axis_size("replica")
    shards_count = lax.axis_size("fsdp")
    local_rows, columns = base_weights.shape
    rows = local_rows // replicas
    groups = 2 * HALF_GROUPS
    width = columns // groups
    total = float(local_rows * shards_count * columns)
    dims = (replicas, shards_count, rows, columns, groups, total)
    most = max(grid_sides(replicas))
    dma = pltpu.SemaphoreType.DMA
    blocks = (groups, replicas, rows, width)
    anywhere = pl.BlockSpec(memory_space=pl.ANY)
    vmem = pl.BlockSpec(memory_space=pltpu.VMEM)
    return pl.pallas_call(
        functools.partial(kernel, dims),
        out_shape=(
            jax.ShapeDtypeStruct(base_weights.shape, jnp.float32),
            jax.ShapeDtypeStruct(momentum.shape, jnp.float32),
            jax.ShapeDtypeStruct(inner_weights.shape, jnp.bfloat16),
        ),
        in_specs=[anywhere] * 3,
        out_specs=(vmem, vmem, vmem),
        scratch_shapes=[
            pltpu.VMEM((local_rows, columns), jnp.float32),
            pltpu.VMEM((local_rows, columns), jnp.bfloat16),
            pltpu.VMEM((rows, columns), jnp.float32),
            pltpu.VMEM(blocks, jnp.bfloat16),
            pltpu.VMEM(blocks, jnp.bfloat16),
            pltpu.VMEM((groups, most, rows, width), jnp.bfloat16),
            pltpu.VMEM((rows, columns), jnp.float32),
            pltpu.VMEM(blocks, jnp.bfloat16),
            pltpu.VMEM((8, BLOCK), jnp.float32),
            pltpu.VMEM((replicas, 8, BLOCK), jnp.float32),
            pltpu.VMEM((8, BLOCK), jnp.float32),
            pltpu.VMEM((shards_count, 8, BLOCK), jnp.float32),
            dma((replicas + 1, 2)),
            dma((groups, replicas)),
            dma((groups, replicas)),
            dma((groups, most)),
            dma((groups, most)),
            dma((groups, replicas)),
            dma((groups, replicas)),
            dma((replicas,)),
            dma((replicas,)),
            dma((shards_count,)),
            dma((shards_count,)),
        ],
        compiler_params=pltpu.CompilerParams(collective_id=0, has_side_effects=True),
    )(base_weights, inner_weights, momentum)


def solution(mesh):
    placed = (P("fsdp", None), P("replica", "fsdp", None), P(("fsdp", "replica"), None))
    return jax.shard_map(
        shards,
        mesh=mesh,
        in_specs=placed,
        out_specs=(P("fsdp", None), P(("fsdp", "replica"), None), P("replica", "fsdp", None)),
        check_vma=False,
    )
```

```python
import functools

import jax
import jax.numpy as jnp
from jax import lax
from jax.experimental import pallas as pl
from jax.experimental.pallas import tpu as pltpu
from jax.sharding import PartitionSpec as P

BLOCK = 128
HALF_GROUPS = 2

code_limit = 448.0
outer_rate = 0.7
outer_momentum = 0.9
blend_share = 0.5
clip_rms = 0.02
epsilon = 1e-06

MESH = pl.DeviceIdType.MESH


def decoded_deltas(deltas):
    peaks = jnp.max(jnp.abs(deltas), axis=1, keepdims=True) + epsilon
    rough = peaks * (1.0 / code_limit)
    wide = rough * (2.0**23 + 1.0)
    power = wide - (wide - rough)
    scales = jnp.where(power * code_limit < peaks, power + power, power)
    nudged = deltas * (1.0 + 2.0**-23)
    wide_deltas = nudged * (2.0**20 + 1.0)
    four_bits = wide_deltas - (wide_deltas - nudged)
    shift = scales * (1.5 * 2.0**14)
    fixed_step = (nudged + shift) - shift
    return jnp.where(jnp.abs(deltas) < scales * 2.0**-6, fixed_step, four_bits)


def grid_sides(replicas):
    side = 1 << (replicas.bit_length() // 2)
    while replicas % side:
        side -= 1
    return side, replicas // side


def kernel(
    dims,
    base_hbm, inner_hbm, momentum_hbm,
    new_base, new_momentum, new_inner,
    base_v, inner_v, momentum_v, dec, first, second, grad, update,
    square_mine, square_near, square_row, square_far,
    load_sems, send_one, recv_one, send_two, recv_two, send_all, recv_all,
    near_send, near_recv, far_send, far_recv,
):
    replicas, shards_count, rows, columns, groups, total = dims
    width = columns // groups
    span_x, span_y = grid_sides(replicas)
    tile = min(32, rows)
    me = lax.axis_index("replica")
    row_me = lax.axis_index("fsdp")
    me_x, me_y = lax.rem(me, span_x), me // span_x

    def spans(g):
        return (span_x, span_y) if g % 2 == 0 else (span_y, span_x)

    def owner(g, dp, dq):
        dx, dy = (dp, dq) if g % 2 == 0 else (dq, dp)
        return lax.rem(me_y + dy, span_y) * span_x + lax.rem(me_x + dx, span_x)

    def near(step):
        return lax.rem(me + step, replicas)

    def far(step):
        return lax.rem(row_me + step, shards_count)

    def row_start(index):
        return pl.multiple_of(index * rows, rows)

    load_order = [(dx, dy) for dy in reversed(range(span_y)) for dx in reversed(range(span_x))]
    loads = []
    for at, (dx, dy) in enumerate(load_order):
        here = pl.ds(row_start(owner(0, dx, dy)), rows)
        pair = (
            pltpu.make_async_copy(base_hbm.at[here], base_v.at[here], load_sems.at[at, 0]),
            pltpu.make_async_copy(inner_hbm.at[0, here], inner_v.at[here], load_sems.at[at, 1]),
        )
        for copy in pair:
            copy.start()
        loads.append(pair)
    momentum_load = pltpu.make_async_copy(momentum_hbm, momentum_v, load_sems.at[replicas, 0])
    momentum_load.start()

    barrier = pltpu.get_barrier_semaphore()
    for step in range(1, replicas):
        pl.semaphore_signal(barrier, inc=1, device_id={"replica": near(step)}, device_id_type=MESH)
    for step in range(1, shards_count):
        pl.semaphore_signal(barrier, inc=1, device_id={"fsdp": far(step)}, device_id_type=MESH)

    def encode(g, dp, dq):
        slot = dp * spans(g)[1] + dq
        start = row_start(owner(g, dp, dq))

        @pl.loop(0, rows // tile)
        def _(t):
            at = pl.ds(pl.multiple_of(start + t * tile, tile), tile)
            to = pl.ds(pl.multiple_of(t * tile, tile), tile)
            for c in range(0, width, BLOCK):
                cols = pl.ds(g * width + c, BLOCK)
                deltas = base_v[at, cols] - inner_v[at, cols].astype(jnp.float32)
                dec[g, slot, to, pl.ds(c, BLOCK)] = decoded_deltas(deltas).astype(jnp.bfloat16)

    def copy_one(g, dp, dq):
        slot = dp * spans(g)[1] + dq
        return pltpu.make_async_remote_copy(
            src_ref=dec.at[g, slot], dst_ref=first.at[g, slot],
            send_sem=send_one.at[g, slot], recv_sem=recv_one.at[g, slot],
            device_id={"replica": owner(g, dp, 0)}, device_id_type=MESH,
        )

    def copy_two(g, dq):
        return pltpu.make_async_remote_copy(
            src_ref=dec.at[g, dq], dst_ref=second.at[g, dq],
            send_sem=send_two.at[g, dq], recv_sem=recv_two.at[g, dq],
            device_id={"replica": owner(g, 0, dq)}, device_id_type=MESH,
        )

    def copy_all(g, dp, dq, source):
        np, nq = spans(g)
        slot = ((np - dp) % np) * nq + (source if dp else (nq - dq) % nq)
        return pltpu.make_async_remote_copy(
            src_ref=update.at[g, source if dp else 0], dst_ref=update.at[g, slot],
            send_sem=send_all.at[g, slot], recv_sem=recv_all.at[g, slot],
            device_id={"replica": owner(g, dp, dq)}, device_id_type=MESH,
        )

    waited = set()

    def await_load(g, dp, dq):
        key = (dp, dq) if g % 2 == 0 else (dq, dp)
        if key not in waited:
            waited.add(key)
            for copy in loads[load_order.index(key)]:
                copy.wait()

    sends = []
    greeted = False
    most = max(span_x, span_y)
    for dq in reversed(range(most)):
        for dp in reversed(range(1, most)):
            for g in range(groups):
                np, nq = spans(g)
                if dp < np and dq < nq:
                    await_load(g, dp, dq)
                    encode(g, dp, dq)
                    if not greeted:
                        pl.semaphore_wait(barrier, replicas - 1 + shards_count - 1)
                        greeted = True
                    copy = copy_one(g, dp, dq)
                    copy.start()
                    sends.append(copy)
    for dq in reversed(range(most)):
        for g in range(groups):
            if dq < spans(g)[1]:
                await_load(g, 0, dq)
                encode(g, 0, dq)

    for dq in reversed(range(most)):
        for g in range(groups):
            np, nq = spans(g)
            if dq >= nq:
                continue
            for dp in range(1, np):
                copy_one(g, dp, dq).wait_recv()

            @pl.loop(0, rows // tile)
            def _(t):
                at = pl.ds(pl.multiple_of(t * tile, tile), tile)
                summed = dec[g, dq, at].astype(jnp.float32)
                for dp in range(1, np):
                    summed += first[g, dp * nq + dq, at].astype(jnp.float32)
                if dq:
                    dec[g, dq, at] = summed.astype(jnp.bfloat16)
                else:
                    grad[at, pl.ds(g * width, width)] = summed

            if dq:
                copy = copy_two(g, dq)
                copy.start()
                sends.append(copy)

    squares = jnp.zeros((8, BLOCK), jnp.float32)
    for g in range(groups):
        nq = spans(g)[1]
        for dq in range(1, nq):
            copy_two(g, dq).wait_recv()

        def add(t, squares):
            at = pl.ds(pl.multiple_of(t * tile, tile), tile)
            for c in range(0, width, BLOCK):
                cols = pl.ds(g * width + c, BLOCK)
                summed = grad[at, cols]
                for dq in range(1, nq):
                    summed += second[g, dq, at, pl.ds(c, BLOCK)].astype(jnp.float32)
                outer = summed * (1.0 / replicas)
                grad[at, cols] = outer
                square = outer * outer
                for s in range(0, tile, 8):
                    squares += square[s : s + 8]
            return squares

        squares = lax.fori_loop(0, rows // tile, add, squares)

    square_mine[...] = squares
    near_copies = []
    for step in range(1, replicas):
        copy = pltpu.make_async_remote_copy(
            src_ref=square_mine, dst_ref=square_near.at[step],
            send_sem=near_send.at[step], recv_sem=near_recv.at[step],
            device_id={"replica": near(step)}, device_id_type=MESH,
        )
        copy.start()
        near_copies.append(copy)
    sends += near_copies
    for copy in near_copies:
        copy.wait_recv()
    for step in range(1, replicas):
        squares += square_near[step]
    square_row[...] = squares
    far_copies = []
    for step in range(1, shards_count):
        copy = pltpu.make_async_remote_copy(
            src_ref=square_row, dst_ref=square_far.at[step],
            send_sem=far_send.at[step], recv_sem=far_recv.at[step],
            device_id={"fsdp": far(step)}, device_id_type=MESH,
        )
        copy.start()
        far_copies.append(copy)
    sends += far_copies
    momentum_load.wait()
    for copy in far_copies:
        copy.wait_recv()
    for step in range(1, shards_count):
        squares += square_far[step]
    mean_square = jnp.full((1, BLOCK), jnp.sum(squares), jnp.float32) / total
    clip_factor = jnp.minimum(1.0, clip_rms / jnp.sqrt(mean_square + epsilon))

    for g in range(groups):
        np, nq = spans(g)

        @pl.loop(0, rows // tile)
        def _(t):
            at = pl.ds(pl.multiple_of(t * tile, tile), tile)
            for c in range(0, width, BLOCK):
                cols = pl.ds(g * width + c, BLOCK)
                step_term = clip_factor * grad[at, cols]
                moved = outer_momentum * momentum_v[at, cols] + step_term
                new_momentum[at, cols] = moved
                update[g, 0, at, pl.ds(c, BLOCK)] = (step_term + outer_momentum * moved).astype(
                    jnp.bfloat16
                )

        for dq in range(1, nq):
            copy = copy_all(g, 0, dq, 0)
            copy.start()
            sends.append(copy)
    for g in range(groups):
        for dp in range(1, spans(g)[0]):
            copy = copy_all(g, dp, 0, 0)
            copy.start()
            sends.append(copy)

    def finish(g, dp, dq):
        slot = dp * spans(g)[1] + dq
        start = row_start(owner(g, dp, dq))

        @pl.loop(0, rows // tile)
        def _(t):
            at = pl.ds(pl.multiple_of(start + t * tile, tile), tile)
            to = pl.ds(pl.multiple_of(t * tile, tile), tile)
            cols = pl.ds(g * width, width)
            fresh = base_v[at, cols] - outer_rate * update[g, slot, to].astype(jnp.float32)
            new_base[at, cols] = fresh
            blended = blend_share * inner_v[at, cols].astype(jnp.float32) + (
                1.0 - blend_share
            ) * fresh
            new_inner[0, at, cols] = blended.astype(jnp.bfloat16)

    for g in range(groups):
        finish(g, 0, 0)
    for g in range(groups):
        np, nq = spans(g)
        for dq in range(1, nq):
            copy_all(g, 0, (nq - dq) % nq, 0).wait_recv()
            for dp in range(1, np):
                copy = copy_all(g, dp, 0, dq)
                copy.start()
                sends.append(copy)
            finish(g, 0, dq)
    for dq in range(most):
        for g in range(groups):
            np, nq = spans(g)
            if dq < nq:
                for dp in range(1, np):
                    copy_all(g, (np - dp) % np, 0, dq).wait_recv()
                    finish(g, dp, dq)
    for copy in sends:
        copy.wait_send()


def write_out(*refs):
    sems = refs[-1]
    parts = len(refs) // 2
    copies = [
        pltpu.make_async_copy(refs[i], refs[parts + i], sems.at[i]) for i in range(parts)
    ]
    for copy in copies:
        copy.start()
    for copy in copies:
        copy.wait()


def shards(base_weights, inner_weights, momentum):
    replicas = lax.axis_size("replica")
    shards_count = lax.axis_size("fsdp")
    local_rows, columns = base_weights.shape
    rows = local_rows // replicas
    groups = 2 * HALF_GROUPS
    width = columns // groups
    total = float(local_rows * shards_count * columns)
    dims = (replicas, shards_count, rows, columns, groups, total)
    most = max(grid_sides(replicas))
    dma = pltpu.SemaphoreType.DMA
    blocks = (groups, replicas, rows, width)
    outside = pl.BlockSpec(memory_space=pltpu.HBM)
    vmem = pl.BlockSpec(memory_space=pltpu.VMEM)
    in_hbm = functools.partial(pltpu.with_memory_space_constraint, memory_space=pltpu.HBM)
    in_vmem = functools.partial(pltpu.with_memory_space_constraint, memory_space=pltpu.VMEM)
    held = pl.pallas_call(
        functools.partial(kernel, dims),
        out_shape=(
            pltpu.VMEM(base_weights.shape, jnp.float32),
            pltpu.VMEM(momentum.shape, jnp.float32),
            pltpu.VMEM(inner_weights.shape, jnp.bfloat16),
        ),
        in_specs=[outside] * 3,
        out_specs=(vmem, vmem, vmem),
        scratch_shapes=[
            pltpu.VMEM((local_rows, columns), jnp.float32),
            pltpu.VMEM((local_rows, columns), jnp.bfloat16),
            pltpu.VMEM((rows, columns), jnp.float32),
            pltpu.VMEM(blocks, jnp.bfloat16),
            pltpu.VMEM(blocks, jnp.bfloat16),
            pltpu.VMEM((groups, most, rows, width), jnp.bfloat16),
            pltpu.VMEM((rows, columns), jnp.float32),
            pltpu.VMEM(blocks, jnp.bfloat16),
            pltpu.VMEM((8, BLOCK), jnp.float32),
            pltpu.VMEM((replicas, 8, BLOCK), jnp.float32),
            pltpu.VMEM((8, BLOCK), jnp.float32),
            pltpu.VMEM((shards_count, 8, BLOCK), jnp.float32),
            dma((replicas + 1, 2)),
            dma((groups, replicas)),
            dma((groups, replicas)),
            dma((groups, most)),
            dma((groups, most)),
            dma((groups, replicas)),
            dma((groups, replicas)),
            dma((replicas,)),
            dma((replicas,)),
            dma((shards_count,)),
            dma((shards_count,)),
        ],
        compiler_params=pltpu.CompilerParams(collective_id=0, has_side_effects=True, vmem_limit_bytes=36 * 2**20),
    )(in_hbm(base_weights), in_hbm(inner_weights), in_hbm(momentum))
    return pl.pallas_call(
        write_out,
        out_shape=tuple(jax.ShapeDtypeStruct(part.shape, part.dtype) for part in held),
        in_specs=[vmem] * len(held),
        out_specs=tuple(outside for part in held),
        scratch_shapes=[dma((len(held),))],
        compiler_params=pltpu.CompilerParams(vmem_limit_bytes=2**20),
    )(*[in_vmem(part) for part in held])


def solution(mesh):
    placed = (P("fsdp", None), P("replica", "fsdp", None), P(("fsdp", "replica"), None))
    return jax.shard_map(
        shards,
        mesh=mesh,
        in_specs=placed,
        out_specs=(P("fsdp", None), P(("fsdp", "replica"), None), P("replica", "fsdp", None)),
        check_vma=False,
    )
```

```python
import functools

import jax
import jax.numpy as jnp
from jax import lax
from jax.experimental import pallas as pl
from jax.experimental.pallas import tpu as pltpu
from jax.sharding import PartitionSpec as P

BLOCK = 128
HALF_GROUPS = 4
EARLY_GROUPS = 2
ENCODE_ROWS = 256
PLAIN_ROWS = 64

code_limit = 448.0
outer_rate = 0.7
outer_momentum = 0.9
blend_share = 0.5
clip_rms = 0.02
epsilon = 1e-06

MESH = pl.DeviceIdType.MESH


def decoded_deltas(deltas):
    peaks = jnp.max(jnp.abs(deltas), axis=1, keepdims=True) + epsilon
    rough = peaks * (1.0 / code_limit)
    wide = rough * (2.0**23 + 1.0)
    power = wide - (wide - rough)
    scales = jnp.where(power * code_limit < peaks, power + power, power)
    nudged = deltas * (1.0 + 2.0**-23)
    wide_deltas = nudged * (2.0**20 + 1.0)
    four_bits = wide_deltas - (wide_deltas - nudged)
    shift = scales * (1.5 * 2.0**14)
    fixed_step = (nudged + shift) - shift
    return jnp.where(jnp.abs(deltas) < scales * 2.0**-6, fixed_step, four_bits)


def grid_sides(replicas):
    side = 1 << (replicas.bit_length() // 2)
    while replicas % side:
        side -= 1
    return side, replicas // side


def kernel(
    dims,
    base_hbm, inner_hbm, momentum_hbm,
    new_base, new_momentum, new_inner,
    base_v, inner_v, momentum_v, dec, first, second, grad, update, early,
    square_mine, square_near, square_row, square_far,
    load_sems, send_one, recv_one, send_two, recv_two, send_all, recv_all,
    near_send, near_recv, far_send, far_recv,
):
    replicas, shards_count, rows, columns, groups, total = dims
    width = columns // groups
    span_x, span_y = grid_sides(replicas)
    tile = min(PLAIN_ROWS, rows)
    encode_tile = min(ENCODE_ROWS, rows)
    me = lax.axis_index("replica")
    row_me = lax.axis_index("fsdp")
    me_x, me_y = lax.rem(me, span_x), me // span_x

    def spans(g):
        return (span_x, span_y) if g % 2 == 0 else (span_y, span_x)

    def owner(g, dp, dq):
        dx, dy = (dp, dq) if g % 2 == 0 else (dq, dp)
        return lax.rem(me_y + dy, span_y) * span_x + lax.rem(me_x + dx, span_x)

    def near(step):
        return lax.rem(me + step, replicas)

    def far(step):
        return lax.rem(row_me + step, shards_count)

    def row_start(index):
        return pl.multiple_of(index * rows, rows)

    load_order = [(dx, dy) for dy in reversed(range(span_y)) for dx in reversed(range(span_x))]
    loads = []
    for at, (dx, dy) in enumerate(load_order):
        here = pl.ds(row_start(owner(0, dx, dy)), rows)
        pair = (
            pltpu.make_async_copy(base_hbm.at[here], base_v.at[here], load_sems.at[at, 0]),
            pltpu.make_async_copy(inner_hbm.at[0, here], inner_v.at[here], load_sems.at[at, 1]),
        )
        for copy in pair:
            copy.start()
        loads.append(pair)
    momentum_load = pltpu.make_async_copy(momentum_hbm, momentum_v, load_sems.at[replicas, 0])
    momentum_load.start()

    barrier = pltpu.get_barrier_semaphore()
    for step in range(1, replicas):
        pl.semaphore_signal(barrier, inc=1, device_id={"replica": near(step)}, device_id_type=MESH)
    for step in range(1, shards_count):
        pl.semaphore_signal(barrier, inc=1, device_id={"fsdp": far(step)}, device_id_type=MESH)

    def encode(g, dp, dq):
        slot = dp * spans(g)[1] + dq
        start = row_start(owner(g, dp, dq))

        @pl.loop(0, rows // encode_tile)
        def _(t):
            at = pl.ds(pl.multiple_of(start + t * encode_tile, encode_tile), encode_tile)
            to = pl.ds(pl.multiple_of(t * encode_tile, encode_tile), encode_tile)
            for c in range(0, width, BLOCK):
                cols = pl.ds(g * width + c, BLOCK)
                deltas = base_v[at, cols] - inner_v[at, cols].astype(jnp.float32)
                dec[g, slot, to, pl.ds(c, BLOCK)] = decoded_deltas(deltas).astype(jnp.bfloat16)

    def copy_one(g, dp, dq):
        slot = dp * spans(g)[1] + dq
        return pltpu.make_async_remote_copy(
            src_ref=dec.at[g, slot], dst_ref=first.at[g, slot],
            send_sem=send_one.at[g, slot], recv_sem=recv_one.at[g, slot],
            device_id={"replica": owner(g, dp, 0)}, device_id_type=MESH,
        )

    def copy_two(g, dq):
        return pltpu.make_async_remote_copy(
            src_ref=dec.at[g, dq], dst_ref=second.at[g, dq],
            send_sem=send_two.at[g, dq], recv_sem=recv_two.at[g, dq],
            device_id={"replica": owner(g, 0, dq)}, device_id_type=MESH,
        )

    def copy_all(g, dp, dq, source):
        np, nq = spans(g)
        slot = ((np - dp) % np) * nq + (source if dp else (nq - dq) % nq)
        blocks = early if g < EARLY_GROUPS else update
        return pltpu.make_async_remote_copy(
            src_ref=blocks.at[g, source if dp else 0], dst_ref=blocks.at[g, slot],
            send_sem=send_all.at[g, slot], recv_sem=recv_all.at[g, slot],
            device_id={"replica": owner(g, dp, dq)}, device_id_type=MESH,
        )

    waited = set()

    def await_load(g, dp, dq):
        key = (dp, dq) if g % 2 == 0 else (dq, dp)
        if key not in waited:
            waited.add(key)
            for copy in loads[load_order.index(key)]:
                copy.wait()

    sends = []
    greeted = False
    most = max(span_x, span_y)
    for dq in reversed(range(most)):
        for dp in reversed(range(1, most)):
            for g in range(groups):
                np, nq = spans(g)
                if dp < np and dq < nq:
                    await_load(g, dp, dq)
                    encode(g, dp, dq)
                    if not greeted:
                        pl.semaphore_wait(barrier, replicas - 1 + shards_count - 1)
                        greeted = True
                    copy = copy_one(g, dp, dq)
                    copy.start()
                    sends.append(copy)
    for dq in reversed(range(most)):
        for g in range(groups):
            if dq < spans(g)[1]:
                await_load(g, 0, dq)
                encode(g, 0, dq)

    for dq in reversed(range(most)):
        for g in range(groups):
            np, nq = spans(g)
            if dq >= nq:
                continue
            for dp in range(1, np):
                copy_one(g, dp, dq).wait_recv()

            @pl.loop(0, rows // tile)
            def _(t):
                at = pl.ds(pl.multiple_of(t * tile, tile), tile)
                summed = dec[g, dq, at].astype(jnp.float32)
                for dp in range(1, np):
                    summed += first[g, dp * nq + dq, at].astype(jnp.float32)
                if dq:
                    dec[g, dq, at] = summed.astype(jnp.bfloat16)
                else:
                    grad[at, pl.ds(g * width, width)] = summed

            if dq:
                copy = copy_two(g, dq)
                copy.start()
                sends.append(copy)

    squares = jnp.zeros((8, BLOCK), jnp.float32)
    for g in range(groups):
        nq = spans(g)[1]
        for dq in range(1, nq):
            copy_two(g, dq).wait_recv()

        def add(t, squares):
            at = pl.ds(pl.multiple_of(t * tile, tile), tile)
            for c in range(0, width, BLOCK):
                cols = pl.ds(g * width + c, BLOCK)
                summed = grad[at, cols]
                for dq in range(1, nq):
                    summed += second[g, dq, at, pl.ds(c, BLOCK)].astype(jnp.float32)
                outer = summed * (1.0 / replicas)
                grad[at, cols] = outer
                square = outer * outer
                for s in range(0, tile, 8):
                    squares += square[s : s + 8]
            return squares

        squares = lax.fori_loop(0, rows // tile, add, squares)

    square_mine[...] = squares
    square_near[0] = squares
    near_copies = []
    for step in range(1, replicas):
        copy = pltpu.make_async_remote_copy(
            src_ref=square_mine, dst_ref=square_near.at[step],
            send_sem=near_send.at[step], recv_sem=near_recv.at[step],
            device_id={"replica": near(step)}, device_id_type=MESH,
        )
        copy.start()
        near_copies.append(copy)
    sends += near_copies

    momentum_load.wait()
    for g in range(EARLY_GROUPS):
        @pl.loop(0, rows // tile)
        def _(t):
            at = pl.ds(pl.multiple_of(t * tile, tile), tile)
            cols = pl.ds(g * width, width)
            early[g, 0, 0, at] = grad[at, cols].astype(jnp.bfloat16)
            early[g, 0, 1, at] = momentum_v[at, cols].astype(jnp.bfloat16)

        for dq in range(1, spans(g)[1]):
            copy = copy_all(g, 0, dq, 0)
            copy.start()
            sends.append(copy)
    for g in range(EARLY_GROUPS):
        for dp in range(1, spans(g)[0]):
            copy = copy_all(g, dp, 0, 0)
            copy.start()
            sends.append(copy)

    for copy in near_copies:
        copy.wait_recv()
    squares = square_near[me]
    for at in range(1, replicas):
        squares += square_near[lax.rem(me + replicas - at, replicas)]
    square_row[...] = squares
    square_far[0] = squares
    far_copies = []
    for step in range(1, shards_count):
        copy = pltpu.make_async_remote_copy(
            src_ref=square_row, dst_ref=square_far.at[step],
            send_sem=far_send.at[step], recv_sem=far_recv.at[step],
            device_id={"fsdp": far(step)}, device_id_type=MESH,
        )
        copy.start()
        far_copies.append(copy)
    sends += far_copies

    def pass_on(g):
        np, nq = spans(g)
        for dq in range(1, nq):
            copy_all(g, 0, (nq - dq) % nq, 0).wait_recv()
            for dp in range(1, np):
                copy = copy_all(g, dp, 0, dq)
                copy.start()
                sends.append(copy)

    for g in range(EARLY_GROUPS):
        pass_on(g)
    for copy in far_copies:
        copy.wait_recv()
    squares = square_far[row_me]
    for at in range(1, shards_count):
        squares += square_far[lax.rem(row_me + shards_count - at, shards_count)]
    mean_square = jnp.full((1, BLOCK), jnp.sum(squares), jnp.float32) / total
    clip_factor = jnp.minimum(1.0, clip_rms / jnp.sqrt(mean_square + epsilon))

    def moved_and_change(outer, kept):
        step_term = clip_factor * outer
        moved = outer_momentum * kept + step_term
        return moved, step_term + outer_momentum * moved

    def advance(g):
        @pl.loop(0, rows // tile)
        def _(t):
            at = pl.ds(pl.multiple_of(t * tile, tile), tile)
            for c in range(0, width, BLOCK):
                cols = pl.ds(g * width + c, BLOCK)
                moved, change = moved_and_change(grad[at, cols], momentum_v[at, cols])
                new_momentum[at, cols] = moved
                if g >= EARLY_GROUPS:
                    update[g, 0, at, pl.ds(c, BLOCK)] = change.astype(jnp.bfloat16)

    for g in range(EARLY_GROUPS, groups):
        advance(g)
        for dq in range(1, spans(g)[1]):
            copy = copy_all(g, 0, dq, 0)
            copy.start()
            sends.append(copy)
    for g in range(EARLY_GROUPS, groups):
        for dp in range(1, spans(g)[0]):
            copy = copy_all(g, dp, 0, 0)
            copy.start()
            sends.append(copy)

    def finish(g, dp, dq):
        slot = dp * spans(g)[1] + dq
        start = row_start(owner(g, dp, dq))

        @pl.loop(0, rows // tile)
        def _(t):
            at = pl.ds(pl.multiple_of(start + t * tile, tile), tile)
            to = pl.ds(pl.multiple_of(t * tile, tile), tile)
            for c in range(0, width, BLOCK):
                cols = pl.ds(g * width + c, BLOCK)
                from_cols = pl.ds(c, BLOCK)
                if g < EARLY_GROUPS:
                    _, change = moved_and_change(
                        early[g, slot, 0, to, from_cols].astype(jnp.float32),
                        early[g, slot, 1, to, from_cols].astype(jnp.float32),
                    )
                else:
                    change = update[g, slot, to, from_cols].astype(jnp.float32)
                fresh = base_v[at, cols] - outer_rate * change
                new_base[at, cols] = fresh
                blended = blend_share * inner_v[at, cols].astype(jnp.float32) + (
                    1.0 - blend_share
                ) * fresh
                new_inner[0, at, cols] = blended.astype(jnp.bfloat16)

    def finish_last(g, dq):
        np = spans(g)[0]
        for dp in range(1, np):
            copy_all(g, (np - dp) % np, 0, dq).wait_recv()
            finish(g, dp, dq)

    for g in range(EARLY_GROUPS):
        advance(g)
        for dq in range(spans(g)[1]):
            finish(g, 0, dq)
    for g in range(EARLY_GROUPS, groups):
        finish(g, 0, 0)
    for g in range(EARLY_GROUPS, groups):
        pass_on(g)
    for g in range(EARLY_GROUPS, groups):
        for dq in range(1, spans(g)[1]):
            finish(g, 0, dq)
    for dq in range(most):
        for g in range(groups):
            if dq < spans(g)[1]:
                finish_last(g, dq)
    for copy in sends:
        copy.wait_send()


def write_out(*refs):
    sems = refs[-1]
    parts = len(refs) // 2
    copies = [
        pltpu.make_async_copy(refs[i], refs[parts + i], sems.at[i]) for i in range(parts)
    ]
    for copy in copies:
        copy.start()
    for copy in copies:
        copy.wait()


def shards(base_weights, inner_weights, momentum):
    replicas = lax.axis_size("replica")
    shards_count = lax.axis_size("fsdp")
    local_rows, columns = base_weights.shape
    rows = local_rows // replicas
    groups = 2 * HALF_GROUPS
    width = columns // groups
    total = float(local_rows * shards_count * columns)
    dims = (replicas, shards_count, rows, columns, groups, total)
    most = max(grid_sides(replicas))
    dma = pltpu.SemaphoreType.DMA
    blocks = (groups, replicas, rows, width)
    outside = pl.BlockSpec(memory_space=pltpu.HBM)
    vmem = pl.BlockSpec(memory_space=pltpu.VMEM)
    in_hbm = functools.partial(pltpu.with_memory_space_constraint, memory_space=pltpu.HBM)
    in_vmem = functools.partial(pltpu.with_memory_space_constraint, memory_space=pltpu.VMEM)
    held = pl.pallas_call(
        functools.partial(kernel, dims),
        out_shape=(
            pltpu.VMEM(base_weights.shape, jnp.float32),
            pltpu.VMEM(momentum.shape, jnp.float32),
            pltpu.VMEM(inner_weights.shape, jnp.bfloat16),
        ),
        in_specs=[outside] * 3,
        out_specs=(vmem, vmem, vmem),
        scratch_shapes=[
            pltpu.VMEM((local_rows, columns), jnp.float32),
            pltpu.VMEM((local_rows, columns), jnp.bfloat16),
            pltpu.VMEM((rows, columns), jnp.float32),
            pltpu.VMEM(blocks, jnp.bfloat16),
            pltpu.VMEM(blocks, jnp.bfloat16),
            pltpu.VMEM((groups, most, rows, width), jnp.bfloat16),
            pltpu.VMEM((rows, columns), jnp.float32),
            pltpu.VMEM(blocks, jnp.bfloat16),
            pltpu.VMEM((max(EARLY_GROUPS, 1), replicas, 2, rows, width), jnp.bfloat16),
            pltpu.VMEM((8, BLOCK), jnp.float32),
            pltpu.VMEM((replicas, 8, BLOCK), jnp.float32),
            pltpu.VMEM((8, BLOCK), jnp.float32),
            pltpu.VMEM((shards_count, 8, BLOCK), jnp.float32),
            dma((replicas + 1, 2)),
            dma((groups, replicas)),
            dma((groups, replicas)),
            dma((groups, most)),
            dma((groups, most)),
            dma((groups, replicas)),
            dma((groups, replicas)),
            dma((replicas,)),
            dma((replicas,)),
            dma((shards_count,)),
            dma((shards_count,)),
        ],
        compiler_params=pltpu.CompilerParams(collective_id=0, has_side_effects=True, vmem_limit_bytes=36 * 2**20),
    )(in_hbm(base_weights), in_hbm(inner_weights), in_hbm(momentum))
    return pl.pallas_call(
        write_out,
        out_shape=tuple(jax.ShapeDtypeStruct(part.shape, part.dtype) for part in held),
        in_specs=[vmem] * len(held),
        out_specs=tuple(outside for part in held),
        scratch_shapes=[dma((len(held),))],
        compiler_params=pltpu.CompilerParams(vmem_limit_bytes=2**20),
    )(*[in_vmem(part) for part in held])


def solution(mesh):
    placed = (P("fsdp", None), P("replica", "fsdp", None), P(("fsdp", "replica"), None))
    return jax.shard_map(
        shards,
        mesh=mesh,
        in_specs=placed,
        out_specs=(P("fsdp", None), P(("fsdp", "replica"), None), P("replica", "fsdp", None)),
        check_vma=False,
    )
```

```python
import functools

import jax
import jax.numpy as jnp
from jax import lax
from jax.experimental import pallas as pl
from jax.experimental.pallas import tpu as pltpu
from jax.sharding import PartitionSpec as P

BLOCK = 128
HALF_GROUPS = 4
EARLY_GROUPS = 2
ENCODE_ROWS = 256
PLAIN_ROWS = 128

code_limit = 448.0
outer_rate = 0.7
outer_momentum = 0.9
blend_share = 0.5
clip_rms = 0.02
epsilon = 1e-06

MESH = pl.DeviceIdType.MESH


def decoded_deltas(deltas):
    peaks = jnp.max(jnp.abs(deltas), axis=1, keepdims=True) + epsilon
    rough = peaks * (1.0 / code_limit)
    wide = rough * (2.0**23 + 1.0)
    power = wide - (wide - rough)
    scales = jnp.where(power * code_limit < peaks, power + power, power)
    nudged = deltas * (1.0 + 2.0**-23)
    wide_deltas = nudged * (2.0**20 + 1.0)
    four_bits = wide_deltas - (wide_deltas - nudged)
    shift = scales * (1.5 * 2.0**14)
    fixed_step = (nudged + shift) - shift
    return jnp.where(jnp.abs(deltas) < scales * 2.0**-6, fixed_step, four_bits)


def grid_sides(replicas):
    side = 1 << (replicas.bit_length() // 2)
    while replicas % side:
        side -= 1
    return side, replicas // side


def kernel(
    dims,
    base_hbm, inner_hbm, momentum_hbm,
    new_base, new_momentum, new_inner,
    base_v, inner_v, momentum_v, dec, first, second, grad, update, early,
    square_mine, square_near, square_row, square_far,
    load_sems, send_one, recv_one, send_two, recv_two, send_all, recv_all,
    near_send, near_recv, far_send, far_recv,
):
    replicas, shards_count, rows, columns, groups, total = dims
    width = columns // groups
    span_x, span_y = grid_sides(replicas)
    tile = min(PLAIN_ROWS, rows)
    encode_tile = min(ENCODE_ROWS, rows)
    me = lax.axis_index("replica")
    row_me = lax.axis_index("fsdp")
    me_x, me_y = lax.rem(me, span_x), me // span_x

    def spans(g):
        return (span_x, span_y) if g % 2 == 0 else (span_y, span_x)

    def owner(g, dp, dq):
        dx, dy = (dp, dq) if g % 2 == 0 else (dq, dp)
        return lax.rem(me_y + dy, span_y) * span_x + lax.rem(me_x + dx, span_x)

    def near(step):
        return lax.rem(me + step, replicas)

    def far(step):
        return lax.rem(row_me + step, shards_count)

    def row_start(index):
        return pl.multiple_of(index * rows, rows)

    barrier = pltpu.get_barrier_semaphore()
    for step in range(1, replicas):
        pl.semaphore_signal(barrier, inc=1, device_id={"replica": near(step)}, device_id_type=MESH)
    for step in range(1, shards_count):
        pl.semaphore_signal(barrier, inc=1, device_id={"fsdp": far(step)}, device_id_type=MESH)

    load_order = [(dx, dy) for dy in reversed(range(span_y)) for dx in reversed(range(span_x))]
    loads = []
    for at, (dx, dy) in enumerate(load_order):
        here = pl.ds(row_start(owner(0, dx, dy)), rows)
        pair = (
            pltpu.make_async_copy(base_hbm.at[here], base_v.at[here], load_sems.at[at, 0]),
            pltpu.make_async_copy(inner_hbm.at[0, here], inner_v.at[here], load_sems.at[at, 1]),
        )
        for copy in pair:
            copy.start()
        loads.append(pair)
    momentum_load = pltpu.make_async_copy(momentum_hbm, momentum_v, load_sems.at[replicas, 0])
    momentum_load.start()

    def encode(g, dp, dq):
        slot = dp * spans(g)[1] + dq
        start = row_start(owner(g, dp, dq))

        @pl.loop(0, rows // encode_tile)
        def _(t):
            at = pl.ds(pl.multiple_of(start + t * encode_tile, encode_tile), encode_tile)
            to = pl.ds(pl.multiple_of(t * encode_tile, encode_tile), encode_tile)
            for c in range(0, width, BLOCK):
                cols = pl.ds(g * width + c, BLOCK)
                deltas = base_v[at, cols] - inner_v[at, cols].astype(jnp.float32)
                dec[g, slot, to, pl.ds(c, BLOCK)] = decoded_deltas(deltas).astype(jnp.bfloat16)

    def copy_one(g, dp, dq):
        slot = dp * spans(g)[1] + dq
        return pltpu.make_async_remote_copy(
            src_ref=dec.at[g, slot], dst_ref=first.at[g, slot],
            send_sem=send_one.at[g, slot], recv_sem=recv_one.at[g, slot],
            device_id={"replica": owner(g, dp, 0)}, device_id_type=MESH,
        )

    def copy_two(g, dq):
        return pltpu.make_async_remote_copy(
            src_ref=dec.at[g, dq], dst_ref=second.at[g, dq],
            send_sem=send_two.at[g, dq], recv_sem=recv_two.at[g, dq],
            device_id={"replica": owner(g, 0, dq)}, device_id_type=MESH,
        )

    def copy_all(g, dp, dq, source):
        np, nq = spans(g)
        slot = ((np - dp) % np) * nq + (source if dp else (nq - dq) % nq)
        blocks = early if g < EARLY_GROUPS else update
        return pltpu.make_async_remote_copy(
            src_ref=blocks.at[g, source if dp else 0], dst_ref=blocks.at[g, slot],
            send_sem=send_all.at[g, slot], recv_sem=recv_all.at[g, slot],
            device_id={"replica": owner(g, dp, dq)}, device_id_type=MESH,
        )

    waited = set()

    def await_load(g, dp, dq):
        key = (dp, dq) if g % 2 == 0 else (dq, dp)
        if key not in waited:
            waited.add(key)
            for copy in loads[load_order.index(key)]:
                copy.wait()

    sends = []
    greeted = False
    most = max(span_x, span_y)
    for dq in reversed(range(most)):
        for dp in reversed(range(1, most)):
            for g in range(groups):
                np, nq = spans(g)
                if dp < np and dq < nq:
                    await_load(g, dp, dq)
                    encode(g, dp, dq)
                    if not greeted:
                        pl.semaphore_wait(barrier, replicas - 1 + shards_count - 1)
                        greeted = True
                    copy = copy_one(g, dp, dq)
                    copy.start()
                    sends.append(copy)
    for dq in reversed(range(most)):
        for g in range(groups):
            if dq < spans(g)[1]:
                await_load(g, 0, dq)
                encode(g, 0, dq)

    for dq in reversed(range(most)):
        for g in range(groups):
            np, nq = spans(g)
            if dq >= nq:
                continue
            for dp in range(1, np):
                copy_one(g, dp, dq).wait_recv()

            @pl.loop(0, rows // tile)
            def _(t):
                at = pl.ds(pl.multiple_of(t * tile, tile), tile)
                summed = dec[g, dq, at].astype(jnp.float32)
                for dp in range(1, np):
                    summed += first[g, dp * nq + dq, at].astype(jnp.float32)
                if dq:
                    dec[g, dq, at] = summed.astype(jnp.bfloat16)
                else:
                    grad[at, pl.ds(g * width, width)] = summed

            if dq:
                copy = copy_two(g, dq)
                copy.start()
                sends.append(copy)

    squares = jnp.zeros((8, BLOCK), jnp.float32)
    for g in range(groups):
        nq = spans(g)[1]
        for dq in range(1, nq):
            copy_two(g, dq).wait_recv()

        def add(t, squares):
            at = pl.ds(pl.multiple_of(t * tile, tile), tile)
            for c in range(0, width, BLOCK):
                cols = pl.ds(g * width + c, BLOCK)
                summed = grad[at, cols]
                for dq in range(1, nq):
                    summed += second[g, dq, at, pl.ds(c, BLOCK)].astype(jnp.float32)
                outer = summed * (1.0 / replicas)
                grad[at, cols] = outer
                square = outer * outer
                for s in range(0, tile, 8):
                    squares += square[s : s + 8]
            return squares

        squares = lax.fori_loop(0, rows // tile, add, squares)

    square_mine[...] = squares
    square_near[0] = squares
    near_copies = []
    for step in range(1, replicas):
        copy = pltpu.make_async_remote_copy(
            src_ref=square_mine, dst_ref=square_near.at[step],
            send_sem=near_send.at[step], recv_sem=near_recv.at[step],
            device_id={"replica": near(step)}, device_id_type=MESH,
        )
        copy.start()
        near_copies.append(copy)
    sends += near_copies

    momentum_load.wait()
    for g in range(EARLY_GROUPS):
        @pl.loop(0, rows // tile)
        def _(t):
            at = pl.ds(pl.multiple_of(t * tile, tile), tile)
            cols = pl.ds(g * width, width)
            early[g, 0, 0, at] = grad[at, cols].astype(jnp.bfloat16)
            early[g, 0, 1, at] = momentum_v[at, cols].astype(jnp.bfloat16)

        for dq in range(1, spans(g)[1]):
            copy = copy_all(g, 0, dq, 0)
            copy.start()
            sends.append(copy)
    for g in range(EARLY_GROUPS):
        for dp in range(1, spans(g)[0]):
            copy = copy_all(g, dp, 0, 0)
            copy.start()
            sends.append(copy)

    for copy in near_copies:
        copy.wait_recv()
    squares = square_near[me]
    for at in range(1, replicas):
        squares += square_near[lax.rem(me + replicas - at, replicas)]
    square_row[...] = squares
    square_far[0] = squares
    far_copies = []
    for step in range(1, shards_count):
        copy = pltpu.make_async_remote_copy(
            src_ref=square_row, dst_ref=square_far.at[step],
            send_sem=far_send.at[step], recv_sem=far_recv.at[step],
            device_id={"fsdp": far(step)}, device_id_type=MESH,
        )
        copy.start()
        far_copies.append(copy)
    sends += far_copies

    def pass_on(g):
        np, nq = spans(g)
        for dq in range(1, nq):
            copy_all(g, 0, (nq - dq) % nq, 0).wait_recv()
            for dp in range(1, np):
                copy = copy_all(g, dp, 0, dq)
                copy.start()
                sends.append(copy)

    for g in range(EARLY_GROUPS):
        pass_on(g)
    for copy in far_copies:
        copy.wait_recv()
    squares = square_far[row_me]
    for at in range(1, shards_count):
        squares += square_far[lax.rem(row_me + shards_count - at, shards_count)]
    mean_square = jnp.full((1, BLOCK), jnp.sum(squares), jnp.float32) / total
    clip_factor = jnp.minimum(1.0, clip_rms / jnp.sqrt(mean_square + epsilon))

    def moved_and_change(outer, kept):
        step_term = clip_factor * outer
        moved = outer_momentum * kept + step_term
        return moved, step_term + outer_momentum * moved

    def advance(g):
        @pl.loop(0, rows // tile)
        def _(t):
            at = pl.ds(pl.multiple_of(t * tile, tile), tile)
            for c in range(0, width, BLOCK):
                cols = pl.ds(g * width + c, BLOCK)
                moved, change = moved_and_change(grad[at, cols], momentum_v[at, cols])
                new_momentum[at, cols] = moved
                if g >= EARLY_GROUPS:
                    update[g, 0, at, pl.ds(c, BLOCK)] = change.astype(jnp.bfloat16)

    for g in range(EARLY_GROUPS, groups):
        advance(g)
        for dq in range(1, spans(g)[1]):
            copy = copy_all(g, 0, dq, 0)
            copy.start()
            sends.append(copy)
    for g in range(EARLY_GROUPS, groups):
        for dp in range(1, spans(g)[0]):
            copy = copy_all(g, dp, 0, 0)
            copy.start()
            sends.append(copy)

    def finish(g, dp, dq):
        slot = dp * spans(g)[1] + dq
        start = row_start(owner(g, dp, dq))

        @pl.loop(0, rows // tile)
        def _(t):
            at = pl.ds(pl.multiple_of(start + t * tile, tile), tile)
            to = pl.ds(pl.multiple_of(t * tile, tile), tile)
            for c in range(0, width, BLOCK):
                cols = pl.ds(g * width + c, BLOCK)
                from_cols = pl.ds(c, BLOCK)
                if g < EARLY_GROUPS:
                    _, change = moved_and_change(
                        early[g, slot, 0, to, from_cols].astype(jnp.float32),
                        early[g, slot, 1, to, from_cols].astype(jnp.float32),
                    )
                else:
                    change = update[g, slot, to, from_cols].astype(jnp.float32)
                fresh = base_v[at, cols] - outer_rate * change
                new_base[at, cols] = fresh
                blended = blend_share * inner_v[at, cols].astype(jnp.float32) + (
                    1.0 - blend_share
                ) * fresh
                new_inner[0, at, cols] = blended.astype(jnp.bfloat16)

    def finish_last(g, dq):
        np = spans(g)[0]
        for dp in range(1, np):
            copy_all(g, (np - dp) % np, 0, dq).wait_recv()
            finish(g, dp, dq)

    for g in range(EARLY_GROUPS):
        advance(g)
        for dq in range(spans(g)[1]):
            finish(g, 0, dq)
    for g in range(EARLY_GROUPS, groups):
        finish(g, 0, 0)
    for g in range(EARLY_GROUPS, groups):
        pass_on(g)
    for g in range(EARLY_GROUPS, groups):
        for dq in range(1, spans(g)[1]):
            finish(g, 0, dq)
    for dq in range(most):
        for g in range(groups):
            if dq < spans(g)[1]:
                finish_last(g, dq)
    for copy in sends:
        copy.wait_send()


def write_out(*refs):
    sems = refs[-1]
    parts = len(refs) // 2
    copies = [
        pltpu.make_async_copy(refs[i], refs[parts + i], sems.at[i]) for i in range(parts)
    ]
    for copy in copies:
        copy.start()
    for copy in copies:
        copy.wait()


def shards(base_weights, inner_weights, momentum):
    replicas = lax.axis_size("replica")
    shards_count = lax.axis_size("fsdp")
    local_rows, columns = base_weights.shape
    rows = local_rows // replicas
    groups = 2 * HALF_GROUPS
    width = columns // groups
    total = float(local_rows * shards_count * columns)
    dims = (replicas, shards_count, rows, columns, groups, total)
    most = max(grid_sides(replicas))
    dma = pltpu.SemaphoreType.DMA
    blocks = (groups, replicas, rows, width)
    outside = pl.BlockSpec(memory_space=pltpu.HBM)
    vmem = pl.BlockSpec(memory_space=pltpu.VMEM)
    in_hbm = functools.partial(pltpu.with_memory_space_constraint, memory_space=pltpu.HBM)
    in_vmem = functools.partial(pltpu.with_memory_space_constraint, memory_space=pltpu.VMEM)
    held = pl.pallas_call(
        functools.partial(kernel, dims),
        out_shape=(
            pltpu.VMEM(base_weights.shape, jnp.float32),
            pltpu.VMEM(momentum.shape, jnp.float32),
            pltpu.VMEM(inner_weights.shape, jnp.bfloat16),
        ),
        in_specs=[outside] * 3,
        out_specs=(vmem, vmem, vmem),
        scratch_shapes=[
            pltpu.VMEM((local_rows, columns), jnp.float32),
            pltpu.VMEM((local_rows, columns), jnp.bfloat16),
            pltpu.VMEM((rows, columns), jnp.float32),
            pltpu.VMEM(blocks, jnp.bfloat16),
            pltpu.VMEM(blocks, jnp.bfloat16),
            pltpu.VMEM((groups, most, rows, width), jnp.bfloat16),
            pltpu.VMEM((rows, columns), jnp.float32),
            pltpu.VMEM(blocks, jnp.bfloat16),
            pltpu.VMEM((max(EARLY_GROUPS, 1), replicas, 2, rows, width), jnp.bfloat16),
            pltpu.VMEM((8, BLOCK), jnp.float32),
            pltpu.VMEM((replicas, 8, BLOCK), jnp.float32),
            pltpu.VMEM((8, BLOCK), jnp.float32),
            pltpu.VMEM((shards_count, 8, BLOCK), jnp.float32),
            dma((replicas + 1, 2)),
            dma((groups, replicas)),
            dma((groups, replicas)),
            dma((groups, most)),
            dma((groups, most)),
            dma((groups, replicas)),
            dma((groups, replicas)),
            dma((replicas,)),
            dma((replicas,)),
            dma((shards_count,)),
            dma((shards_count,)),
        ],
        compiler_params=pltpu.CompilerParams(collective_id=0, has_side_effects=True, vmem_limit_bytes=36 * 2**20),
    )(in_hbm(base_weights), in_hbm(inner_weights), in_hbm(momentum))
    return pl.pallas_call(
        write_out,
        out_shape=tuple(jax.ShapeDtypeStruct(part.shape, part.dtype) for part in held),
        in_specs=[vmem] * len(held),
        out_specs=tuple(outside for part in held),
        scratch_shapes=[dma((len(held),))],
        compiler_params=pltpu.CompilerParams(vmem_limit_bytes=2**20),
    )(*[in_vmem(part) for part in held])


def solution(mesh):
    placed = (P("fsdp", None), P("replica", "fsdp", None), P(("fsdp", "replica"), None))
    return jax.shard_map(
        shards,
        mesh=mesh,
        in_specs=placed,
        out_specs=(P("fsdp", None), P(("fsdp", "replica"), None), P("replica", "fsdp", None)),
        check_vma=False,
    )
```
